32 devices in a mesh: data: 1 (over z), tp: 4 (over y), ep: 8 (over x, core).
Axes of the slice: x: 4, y: 4, z: 1, core: 2. Of those that a mesh axis runs over, the one named last changes fastest.
The devices are a block of a 4x4x8 slice.
Arguments:
- tokens: bfloat16 [4096, 2560], P(('data', 'ep', 'tp'))
- expert_ids: int32 [4096, 6], P(('data', 'ep', 'tp'))
- gate_vals: float32 [4096, 6], P(('data', 'ep', 'tp'))
- slot_ids: int32 [4096, 6], P(('data', 'ep', 'tp'))
- send_counts: int32 [32, 64], P(('data', 'ep', 'tp'))
- shared_w1: bfloat16 [2560, 3072], P(None, 'tp')
- shared_w3: bfloat16 [2560, 3072], P(None, 'tp')
- shared_w2: bfloat16 [3072, 2560], P('tp')
- expert_w1: bfloat16 [64, 2560, 1536], P('ep')
- expert_w3: bfloat16 [64, 2560, 1536], P('ep')
- expert_w2: bfloat16 [64, 1536, 2560], P('ep')
Outputs:
- output: bfloat16 [4096, 2560], P(('data', 'ep', 'tp'))
All inputs are finite; a program needn't handle non-finite values.
Results may differ from the reference program's by a relative error of at most 0.001.
Values are sent between devices in bfloat16 or wider.
A program may use at most 768 MiB of HBM per device.

```python
import jax
import jax.numpy as jnp
from jax import lax

EP = 8
TP = 4
TOKENS_DEV = 128
D = 2560
FS = 3072
FF = 1536
EXPERTS = 64
TOP = 6
HOT = 8
CAP = 48

N_SRC = EP * TP
TOKENS = TOKENS_DEV * N_SRC


def draw_routing(route_key):
    key_hot, key_wts, key_perm = jax.random.split(route_key, 3)
    experts = jnp.arange(EXPERTS, dtype=jnp.int32)
    offset = jax.random.randint(key_hot, (), 0, EXPERTS, dtype=jnp.int32)
    is_hot = ((experts - offset) % EXPERTS) < HOT
    weights = jax.random.randint(key_wts, (N_SRC, EXPERTS), 1, 3, dtype=jnp.int32)
    cum_wts = jnp.cumsum(jnp.where(is_hot[None, :], 0, weights), axis=1)
    cold_total = TOKENS_DEV * TOP - HOT * CAP
    bounds = (cold_total * cum_wts) // cum_wts[:, -1:]
    prev_bounds = jnp.concatenate([jnp.zeros((N_SRC, 1), jnp.int32), bounds[:, :-1]], axis=1)
    counts = jnp.where(is_hot[None, :], CAP, bounds - prev_bounds).astype(jnp.int32)
    run_ends = jnp.cumsum(counts, axis=1)
    copy_pos = jnp.arange(TOKENS_DEV * TOP, dtype=jnp.int32)
    expert_of = jax.vmap(lambda end_row: jnp.searchsorted(end_row, copy_pos, side="right"))(run_ends).astype(jnp.int32)
    slot_of = copy_pos[None, :] - jnp.take_along_axis(run_ends - counts, expert_of, axis=1)
    expert_of = expert_of.reshape(N_SRC, TOP, TOKENS_DEV).transpose(0, 2, 1)
    slot_of = slot_of.reshape(N_SRC, TOP, TOKENS_DEV).transpose(0, 2, 1)
    tok_perms = jax.vmap(lambda perm_key: jax.random.permutation(perm_key, TOKENS_DEV))(jax.random.split(key_perm, N_SRC))
    expert_of = jnp.take_along_axis(expert_of, tok_perms[:, :, None], axis=1)
    slot_of = jnp.take_along_axis(slot_of, tok_perms[:, :, None], axis=1)
    return expert_of.reshape(TOKENS, TOP).astype(jnp.int32), slot_of.reshape(TOKENS, TOP).astype(jnp.int32), counts


def scaled_normal(weight_key, shape, fan_in):
    return (jax.random.normal(weight_key, shape, jnp.float32) * fan_in ** -0.5).astype(jnp.bfloat16)


def setup_inputs(seed: int = 0, part: int = 0) -> dict:
    base_key = jax.random.key(seed)
    part_key = jax.random.fold_in(base_key, part)
    key_x, key_gate, key_route = jax.random.split(part_key, 3)
    weight_keys = jax.random.split(jax.random.key(seed + 1), 6)
    tokens = jax.random.normal(key_x, (TOKENS, D), jnp.float32).astype(jnp.bfloat16)
    expert_ids, slot_ids, send_counts = draw_routing(key_route)
    gate_vals = jax.random.uniform(key_gate, (TOKENS, TOP), jnp.float32, 0.5, 1.5) * TOP ** -0.5
    return {
        "tokens": tokens,
        "expert_ids": expert_ids,
        "gate_vals": gate_vals,
        "slot_ids": slot_ids,
        "send_counts": send_counts,
        "shared_w1": scaled_normal(weight_keys[0], (D, FS), D),
        "shared_w3": scaled_normal(weight_keys[1], (D, FS), D),
        "shared_w2": scaled_normal(weight_keys[2], (FS, D), FS),
        "expert_w1": scaled_normal(weight_keys[3], (EXPERTS, D, FF), D),
        "expert_w3": scaled_normal(weight_keys[4], (EXPERTS, D, FF), D),
        "expert_w2": scaled_normal(weight_keys[5], (EXPERTS, FF, D), FF),
    }


def shared_block(tok_block, shared_w1, shared_w3, shared_w2):
    pre_gate = jnp.dot(tok_block, shared_w1, preferred_element_type=jnp.float32)
    pre_up = jnp.dot(tok_block, shared_w3, preferred_element_type=jnp.float32)
    hidden = (jax.nn.silu(pre_gate) * pre_up).astype(jnp.bfloat16)
    return jnp.dot(hidden, shared_w2, preferred_element_type=jnp.float32)


def reference(tokens, expert_ids, gate_vals, slot_ids, send_counts, shared_w1, shared_w3, shared_w2, expert_w1, expert_w3, expert_w2):
    tok_blocks = tokens.reshape(N_SRC, TOKENS_DEV, D)
    shared_out = lax.map(lambda tok_block: shared_block(tok_block, shared_w1, shared_w3, shared_w2), tok_blocks).reshape(TOKENS, D)
    src_ids = jnp.arange(TOKENS, dtype=jnp.int32) // TOKENS_DEV
    row_limit = send_counts[src_ids[:, None], expert_ids]
    kept_mask = (slot_ids >= 0) & (slot_ids < row_limit)
    n_rows = N_SRC * EXPERTS * CAP
    dest_row = jnp.where(kept_mask, (src_ids[:, None] * EXPERTS + expert_ids) * CAP + slot_ids, n_rows)
    copy_ids = jnp.arange(TOKENS * TOP, dtype=jnp.int32)
    owner_ids = jnp.full((n_rows,), TOKENS * TOP, jnp.int32).at[dest_row.reshape(-1)].set(copy_ids, mode="drop")
    owner_ids = owner_ids.reshape(N_SRC, EXPERTS, CAP).transpose(1, 0, 2).reshape(EXPERTS, N_SRC * CAP)
    flat_gates = gate_vals.reshape(-1)

    def expert_step(running, step_in):
        w_in, w_up, w_out, own_ids = step_in
        tok_of = own_ids // TOP
        expert_rows = jnp.take(tokens, tok_of, axis=0, mode="fill", fill_value=0)
        pre_gate = jnp.dot(expert_rows, w_in, preferred_element_type=jnp.float32)
        pre_up = jnp.dot(expert_rows, w_up, preferred_element_type=jnp.float32)
        hidden = (jax.nn.silu(pre_gate) * pre_up).astype(jnp.bfloat16)
        routed = jnp.dot(hidden, w_out, preferred_element_type=jnp.float32).astype(jnp.bfloat16)
        weight = jnp.take(flat_gates, own_ids, mode="fill", fill_value=0)
        running = running.at[tok_of].add(weight[:, None] * routed.astype(jnp.float32), mode="drop")
        return running, None

    routed_sum = lax.scan(expert_step, jnp.zeros((TOKENS, D), jnp.float32), (expert_w1, expert_w3, expert_w2, owner_ids))[0]
    return (tokens.astype(jnp.float32) + shared_out + routed_sum).astype(jnp.bfloat16)
```

```python
import functools

import jax
import jax.numpy as jnp
from jax import lax
from jax.experimental import pallas as pl
from jax.experimental.pallas import tpu as pltpu
from jax.sharding import PartitionSpec as P

CAP_FACTOR = 4
BF = jnp.bfloat16
F32 = jnp.float32
MESH = pl.DeviceIdType.MESH
BLK = 256
META = 16


def capacity_rows(n_tok, top_k, n_exp):
    return min(n_tok, ((CAP_FACTOR * n_tok * top_k // n_exp + 7) // 8) * 8)


def silu_mul(g, u):
    return (g * (1.0 / (1.0 + jnp.exp(-g))) * u).astype(BF)


def dot(a, b):
    return jnp.dot(a, b, preferred_element_type=F32)


def layer_kernel(cfg, tok, meta, ws1, ws3, ws2, w1, w3, w2, out,
                 hr, xg, mg, pb, sb, d2d, far, fin, yfar, yfin, acc, sh, gu, gm, ring,
                 own_sem, xs, xr, ps, pr, ms, mr, ys, yr, wsem,
                 ysend, yrecv, dsend, drecv, fsend, frecv, nsend, nrecv):
    EP, TP, NT, D, FF, FS, NL, CAP, TOPK, NS = cfg
    ROWS = EP * CAP
    LROWS = NL * CAP
    H = NT // 2
    NX = EP // 2
    NB = D // BLK
    C1 = FF // BLK
    Q1 = NL * C1
    PAIRS = NL // 2
    Q2 = NB * PAIRS
    SA = FS // BLK
    SB = D // (2 * BLK)

    me = lax.axis_index("ep")
    ty = lax.axis_index("tp")
    cx = me // 2
    cc = me % 2
    mate = cx * 2 + (1 - cc)
    rx = (cx + 1) % NX
    lx = (cx + NX - 1) % NX
    fx = (cx + 2) % NX
    right = {"ep": rx * 2 + cc}
    left = {"ep": lx * 2 + cc}
    up = {"tp": (ty + 1) % TP}
    down = {"tp": (ty + TP - 1) % TP}
    partner = {"ep": mate}

    def remote(src, dst, ssem, rsem, dev):
        return pltpu.make_async_remote_copy(src_ref=src, dst_ref=dst, send_sem=ssem, recv_sem=rsem, device_id=dev, device_id_type=MESH)

    def wpair(slot, ra, rb, n):
        return (pltpu.make_async_copy(ra, ring.at[slot, pl.ds(0, n), pl.ds(0, BLK)], wsem.at[slot, 0]),
                pltpu.make_async_copy(rb, ring.at[slot, pl.ds(0, n), pl.ds(BLK, BLK)], wsem.at[slot, 1]))

    def cols(i, w=BLK):
        return pl.ds(pl.multiple_of(i * w, w), w)

    def chunk_a(i):
        return wpair(i % NS, ws1.at[:, cols(i)], ws3.at[:, cols(i)], D)

    def chunk_b(i):
        return wpair((i + SA) % NS, ws2.at[:, cols(2 * i)], ws2.at[:, cols(2 * i + 1)], FS)

    def chunk_1(q):
        e, n = q // C1, q % C1
        return wpair((q + SA + SB) % NS, w1.at[e, :, cols(n)], w3.at[e, :, cols(n)], D)

    def chunk_2(q):
        b, p = q // PAIRS, q % PAIRS
        return wpair((q + SA + SB + Q1) % NS, w2.at[2 * p, :, cols(b)], w2.at[2 * p + 1, :, cols(b)], FF)

    def start(pair):
        pair[0].start()
        pair[1].start()

    def wait(pair):
        pair[0].wait()
        pair[1].wait()

    total = SA + SB + Q1 + Q2

    def start_at(i):
        bounds = ((0, SA, chunk_a), (SA, SA + SB, chunk_b), (SA + SB, SA + SB + Q1, chunk_1), (SA + SB + Q1, total, chunk_2))
        for lo, hi, fn in bounds:
            if isinstance(i, int):
                if lo <= i < hi:
                    start(fn(i - lo))
            else:
                @pl.when((i >= lo) & (i < hi))
                def _(fn=fn, lo=lo):
                    start(fn(i - lo))

    own = pltpu.make_async_copy(tok, xg.at[me], own_sem)
    own.start()
    for i in range(NS - 1):
        start_at(i)

    barrier = pltpu.get_barrier_semaphore()
    for d in range(1, EP):
        pl.semaphore_signal(barrier, inc=1, device_id={"ep": (me + d) % EP}, device_id_type=MESH)
    for dev in (up, down):
        pl.semaphore_signal(barrier, inc=1, device_id=dev, device_id_type=MESH)
    mg[me] = meta[...]
    own.wait()
    pl.semaphore_wait(barrier, EP + 1)

    lo_h, hi_h, all_h = pl.ds(0, H), pl.ds(H, H), pl.ds(0, NT)

    def xpart(dx, part):
        return xg.at[((cx + dx + NX) % NX) * 2 + cc, part, :]

    def xsend(k, dx, part, dev):
        ref = xpart(dx, part)
        return remote(ref, ref, xs.at[k], xr.at[k], dev)

    x_r0 = xsend(0, 0, lo_h, right)
    x_r1 = xsend(1, 0, hi_h, right)
    x_l1 = xsend(2, 0, hi_h, left)
    x_l0 = xsend(3, 0, lo_h, left)
    x_fr = xsend(4, -1, lo_h, right)
    x_fl = xsend(5, 1, hi_h, left)

    def psend(k, dx, part):
        ref = xpart(dx, part)
        return remote(ref, ref, ps.at[k], pr.at[k], partner)

    p_own = psend(0, 0, all_h)
    p_l = psend(1, -1, all_h)
    p_r = psend(2, 1, all_h)
    p_f0 = psend(3, 2, lo_h)
    p_f1 = psend(4, 2, hi_h)

    def ypart(j, part_start, n):
        return hr.at[0, pl.ds(j * NT + part_start, n), :]

    y_r0 = remote(xg.at[me, lo_h, :], ypart(0, 0, H), ys.at[0], yr.at[0], up)
    y_r1 = remote(xg.at[me, hi_h, :], ypart(0, H, H), ys.at[1], yr.at[1], up)
    y_l1 = remote(xg.at[me, hi_h, :], ypart(1, H, H), ys.at[2], yr.at[2], down)
    y_l0 = remote(xg.at[me, lo_h, :], ypart(1, 0, H), ys.at[3], yr.at[3], down)
    y_fr = remote(ypart(0, 0, H), ypart(2, 0, H), ys.at[4], yr.at[4], up)
    y_fl = remote(ypart(1, H, H), ypart(2, H, H), ys.at[5], yr.at[5], down)

    metas = [remote(mg.at[me], mg.at[me], ms.at[d - 1], mr.at[d - 1], {"ep": (me + d) % EP}) for d in range(1, EP)]

    for c in metas:
        c.start()
    for c in (x_r0, x_l1, y_r0, y_l1, p_own, x_r1, x_l0, y_r1, y_l0):
        c.start()

    row_id = lax.broadcasted_iota(jnp.int32, (LROWS, NT), 0).astype(F32) + (me * LROWS).astype(F32)

    def gather(k, _):
        k2 = k // 2
        dx = (3 * k2 + 3 * (k2 // 2) - 2 * (k2 // 3)) % NX
        s = ((cx + dx) % NX) * 2 + (cc + k) % 2
        m = mg[s]
        pick = jnp.zeros((LROWS, NT), F32)
        wgt = jnp.zeros((LROWS, NT), F32)
        for j in range(TOPK):
            hit = m[j:j + 1, :] == row_id
            pick = jnp.where(hit, 1.0, pick)
            wgt = wgt + jnp.where(hit, m[8 + j:9 + j, :], 0.0)
        pick = pick.astype(BF)
        wt = jnp.transpose(wgt)
        hi = wt.astype(BF)
        rest = wt - hi.astype(F32)
        mid = rest.astype(BF)
        low = (rest - mid.astype(F32)).astype(BF)
        gm[s, 0:NT, :] = hi
        gm[s, NT:2 * NT, :] = mid
        gm[s, 2 * NT:3 * NT, :] = low
        place = pl.ds(pl.multiple_of(s * CAP, CAP), CAP)
        for n in range(D // 512):
            part = slice(n * 512, (n + 1) * 512)
            got = dot(pick, xg[s, :, part]).astype(BF)
            for e in range(NL):
                hr[e + 1, place, part] = got[e * CAP:(e + 1) * CAP, :]
        return 0

    for c in metas:
        c.wait_recv()
    lax.fori_loop(0, 1, gather, 0)

    x_r0.wait_recv()
    x_fr.start()
    x_l1.wait_recv()
    x_fl.start()
    y_r0.wait_recv()
    y_fr.start()
    y_l1.wait_recv()
    y_fl.start()
    x_r1.wait_recv()
    p_l.start()
    x_l0.wait_recv()
    p_r.start()
    y_r1.wait_recv()
    y_l0.wait_recv()
    p_own.wait_recv()
    p_l.wait_recv()
    p_r.wait_recv()
    lax.fori_loop(1, 6, gather, 0)
    x_fr.wait_recv()
    p_f0.start()
    x_fl.wait_recv()
    p_f1.start()
    y_fr.wait_recv()
    y_fl.wait_recv()

    def shared_in(n, _):
        wait(chunk_a(n))
        slot = n % NS
        start_at(n - 1 + NS)
        a = dot(hr[0], ring[slot])
        b = dot(xg[me], ring[slot])
        sh[pl.ds(NT, 3 * NT), cols(n)] = silu_mul(a[:, :BLK], a[:, BLK:])
        sh[pl.ds(0, NT), cols(n)] = silu_mul(b[:, :BLK], b[:, BLK:])
        return 0

    lax.fori_loop(0, SA, shared_in, 0)

    def shared_out(i, _):
        wait(chunk_b(i))
        slot = (i + SA) % NS
        start_at(i + SA - 1 + NS)
        r = dot(sh[...], ring[slot, pl.ds(0, FS), :])
        here = pl.ds(pl.multiple_of(i * 2 * BLK, 2 * BLK), 2 * BLK)
        acc[:, here] = xg[me, :, here].astype(F32) + r[0:NT, :]
        for j in range(3):
            for h in range(2):
                pb[2 * i + h, j] = r[(j + 1) * NT:(j + 2) * NT, h * BLK:(h + 1) * BLK]
        return 0

    lax.fori_loop(0, SB, shared_out, 0)

    def y_half(k, dev):
        return remote(pb.at[:, 2, pl.ds(k * H, H), :], yfar.at[k], ysend.at[k], yrecv.at[k], dev)

    def y_full(k, j, dev):
        return remote(pb.at[:, j], yfin.at[k], ysend.at[2 + k], yrecv.at[2 + k], dev)

    y_halves = (y_half(0, up), y_half(1, down))
    y_fulls = (y_full(0, 1, up), y_full(1, 0, down))
    for c in y_halves:
        c.start()

    p_f0.wait_recv()
    p_f1.wait_recv()
    lax.fori_loop(6, EP, gather, 0)

    def y_step2():
        for c in y_halves:
            c.wait()

        def add(i, _):
            pb[i, 1, 0:H, :] += yfar[0, i]
            pb[i, 0, H:NT, :] += yfar[1, i]
            return 0

        lax.fori_loop(0, NB, add, 0)
        for c in y_fulls:
            c.start()

    def y_step3():
        for c in y_fulls:
            c.wait()

        def add(i, _):
            acc[:, cols(i)] += yfin[0, i] + yfin[1, i]
            return 0

        lax.fori_loop(0, NB, add, 0)

    y_fr.wait_send()
    y_fl.wait_send()

    def finish(e, n):
        g = gu[n % 2]
        hr[e, :, n * BLK:(n + 1) * BLK] = silu_mul(g[:, :BLK], g[:, BLK:])

    def first(e, _):
        @pl.when(e == 2)
        def _():
            y_step2()

        @pl.when(e == NL - 1)
        def _():
            y_step3()

        for n in range(C1):
            q = e * C1 + n
            wait(chunk_1(q))
            start_at(SA + SB + q - 1 + NS)
            gu[n % 2] = dot(hr[e + 1], ring[(q + SA + SB) % NS])
            if n:
                finish(e, n - 1)
            else:
                finish(jnp.maximum(e - 1, 0), C1 - 1)
        return 0

    lax.fori_loop(0, NL, first, 0)
    finish(NL - 1, C1 - 1)

    def to_mate(b):
        return remote(sb.at[b % 2], d2d.at[b], dsend.at[b], drecv.at[b], partner)

    def half(b, k, dev):
        return remote(pb.at[b, fx, pl.ds(k * H, H), :], far.at[k, b], fsend.at[k, b], frecv.at[k, b], dev)

    def full(b, k, x, dev):
        return remote(pb.at[b, x], fin.at[k, b], nsend.at[k, b], nrecv.at[k, b], dev)

    def step_b(b):
        to_mate(b).wait_recv()
        pb[b] += d2d[b]
        half(b, 0, right).start()
        half(b, 1, left).start()

    def step_c(b):
        half(b, 0, right).wait_recv()
        half(b, 1, left).wait_recv()
        pb[b, rx, 0:H, :] += far[0, b]
        pb[b, lx, H:NT, :] += far[1, b]
        full(b, 0, rx, right).start()
        full(b, 1, lx, left).start()

    def step_d(b, _):
        full(b, 0, rx, right).wait_recv()
        full(b, 1, lx, left).wait_recv()
        out[:, cols(b)] = (acc[:, cols(b)] + pb[b, cx] + fin[0, b] + fin[1, b]).astype(BF)
        return 0

    def combine(b, par, dest):
        for x in range(NX):
            s = x * 2 + par
            place = pl.ds(pl.multiple_of(s * CAP, CAP), CAP)
            r = jnp.concatenate([hr[e, place, FF:FF + BLK] for e in range(NL)], axis=0)
            v = dot(gm[s], r)
            dest[x] = v[0:NT] + (v[NT:2 * NT] + v[2 * NT:3 * NT])

    def second(b, _):
        for p in range(PAIRS):
            q = b * PAIRS + p
            wait(chunk_2(q))
            start_at(SA + SB + Q1 + q - 1 + NS)
            slot = (q + SA + SB + Q1) % NS
            for h in range(2):
                e = 2 * p + h
                hr[e, :, FF:FF + BLK] = dot(hr[e, :, 0:FF], ring[slot, 0:FF, h * BLK:(h + 1) * BLK]).astype(BF)
            if p == 1:
                @pl.when(b >= 1)
                def _():
                    step_b(b - 1)

                @pl.when(b >= 2)
                def _():
                    step_c(b - 2)

        @pl.when(b >= 2)
        def _():
            to_mate(b - 2).wait_send()

        combine(b, 1 - cc, sb.at[b % 2])
        to_mate(b).start()
        combine(b, cc, pb.at[b])
        return 0

    lax.fori_loop(0, NB, second, 0)
    step_b(NB - 1)
    step_c(NB - 2)
    step_c(NB - 1)
    lax.fori_loop(0, NB, step_d, 0)

    for c in metas:
        c.wait_send()
    for c in (x_r0, x_r1, x_l1, x_l0, x_fr, x_fl, p_own, p_l, p_r, p_f0, p_f1, y_r0, y_r1, y_l1, y_l0):
        c.wait_send()
    to_mate(NB - 2).wait_send()
    to_mate(NB - 1).wait_send()

    def drain(b, _):
        half(b, 0, right).wait_send()
        half(b, 1, left).wait_send()
        full(b, 0, rx, right).wait_send()
        full(b, 1, lx, left).wait_send()
        return 0

    lax.fori_loop(0, NB, drain, 0)


def solution(mesh):
    ep_size = mesh.shape["ep"]
    tp_size = mesh.shape["tp"]
    row_spec = P(("data", "ep", "tp"), None)
    expert_spec = P("ep", None, None)

    def layer_body(tokens, expert_ids, gate_vals, slot_ids, send_counts, shared_w1, shared_w3, shared_w2, expert_w1, expert_w3, expert_w2):
        n_tok, d_model = tokens.shape
        top_k = expert_ids.shape[1]
        n_local, _, width = expert_w1.shape
        shared_width = shared_w1.shape[1]
        n_exp = n_local * ep_size
        capacity = capacity_rows(n_tok, top_k, n_exp)
        n_rows = n_exp * capacity

        same = expert_ids[:, :, None] == jnp.arange(n_exp, dtype=jnp.int32)[None, None, :]
        row_limit = jnp.sum(jnp.where(same, send_counts[0][None, None, :], 0), axis=-1)
        kept_mask = (slot_ids >= 0) & (slot_ids < row_limit)
        dest_row = jnp.where(kept_mask, expert_ids * capacity + slot_ids, n_rows).astype(F32)
        gate_eff = jnp.where(kept_mask, gate_vals, 0.0)
        pad = ((0, META // 2 - top_k), (0, 0))
        meta = jnp.concatenate([jnp.pad(dest_row.T, pad), jnp.pad(gate_eff.T, pad)], axis=0)

        ns = 4
        nb = d_model // BLK
        local_rows = n_local * capacity
        cfg = (ep_size, tp_size, n_tok, d_model, width, shared_width, n_local, capacity, top_k, ns)
        half = n_tok // 2
        nx = ep_size // 2
        hbm = pl.BlockSpec(memory_space=pl.ANY)
        vmem = pl.BlockSpec(memory_space=pltpu.VMEM)
        dma = pltpu.SemaphoreType.DMA
        return pl.pallas_call(
            functools.partial(layer_kernel, cfg),
            out_shape=jax.ShapeDtypeStruct((n_tok, d_model), BF),
            in_specs=[hbm, vmem] + [hbm] * 6,
            out_specs=vmem,
            scratch_shapes=[
                pltpu.VMEM((n_local + 1, ep_size * capacity, d_model), BF),
                pltpu.VMEM((ep_size, n_tok, d_model), BF),
                pltpu.VMEM((ep_size, META, n_tok), F32),
                pltpu.VMEM((nb, nx, n_tok, BLK), F32),
                pltpu.VMEM((2, nx, n_tok, BLK), F32),
                pltpu.VMEM((nb, nx, n_tok, BLK), F32),
                pltpu.VMEM((2, nb, half, BLK), F32),
                pltpu.VMEM((2, nb, n_tok, BLK), F32),
                pltpu.VMEM((2, nb, half, BLK), F32),
                pltpu.VMEM((2, nb, n_tok, BLK), F32),
                pltpu.VMEM((n_tok, d_model), F32),
                pltpu.VMEM((tp_size * n_tok, shared_width), BF),
                pltpu.VMEM((2, ep_size * capacity, 2 * BLK), F32),
                pltpu.VMEM((ep_size, 3 * n_tok, local_rows), BF),
                pltpu.VMEM((ns, d_model, 2 * BLK), BF),
                dma, dma((6,)), dma((6,)), dma((5,)), dma((5,)), dma((ep_size - 1,)), dma((ep_size - 1,)),
                dma((6,)), dma((6,)), dma((ns, 2)),
                dma((4,)), dma((4,)), dma((nb,)), dma((nb,)), dma((2, nb)), dma((2, nb)), dma((2, nb)), dma((2, nb)),
            ],
            compiler_params=pltpu.CompilerParams(collective_id=0, has_side_effects=True, vmem_limit_bytes=67043328),
            cost_estimate=pl.CostEstimate(flops=80_000_000_000, bytes_accessed=200_000_000, transcendentals=0),
            name="moe_layer",
        )(tokens, meta, shared_w1, shared_w3, shared_w2, expert_w1, expert_w3, expert_w2)

    return jax.shard_map(
        layer_body,
        mesh=mesh,
        in_specs=(row_spec, row_spec, row_spec, row_spec, row_spec, P(None, "tp"), P(None, "tp"), P("tp", None), expert_spec, expert_spec, expert_spec),
        out_specs=row_spec,
        check_vma=False,
    )
```

```python
import functools

import jax
import jax.numpy as jnp
from jax import lax
from jax.experimental import pallas as pl
from jax.experimental.pallas import tpu as pltpu
from jax.sharding import PartitionSpec as P

CAP_FACTOR = 4
BF = jnp.bfloat16
F32 = jnp.float32
MESH = pl.DeviceIdType.MESH
BLK = 256
META = 16


def capacity_rows(n_tok, top_k, n_exp):
    return min(n_tok, ((CAP_FACTOR * n_tok * top_k // n_exp + 7) // 8) * 8)


def silu_mul(g, u):
    return (g * (1.0 / (1.0 + jnp.exp(-g))) * u).astype(BF)


def dot(a, b):
    return jnp.dot(a, b, preferred_element_type=F32)


def layer_kernel(cfg, tok, ids, slots, gates, counts, ws1, ws3, ws2, w1, w3, w2, out,
                 hr, xg, yg, mg, pb, sb, d2d, far, fin, yfar, acc, sh, gu, gm, ring,
                 own_sem, xs, xr, ps, pr, ms, mr, ys, yr, wsem,
                 ysend, yrecv, dsend, drecv, fsend, frecv, nsend, nrecv):
    EP, TP, NT, D, FF, FS, NL, CAP, TOPK, NS = cfg
    ROWS = EP * CAP
    LROWS = NL * CAP
    H = NT // 2
    NX = EP // 2
    NB = D // BLK
    C1 = FF // BLK
    Q1 = NL * C1
    PAIRS = NL // 2
    Q2 = NB * PAIRS
    SA = FS // BLK
    SB = D // (2 * BLK)
    K1 = D // BLK
    K2 = FF // BLK
    KG = -(-3 * LROWS // BLK)
    GK = KG * BLK
    KS = FS // BLK
    NE = NL // 2
    G1 = C1 // 3
    G2 = PAIRS // 2
    QE = NE * C1
    PR = 2 * CAP
    O_A = QE
    O_B = O_A + SA
    O_1 = O_B + SB
    O_2 = O_1 + Q1
    total = O_2 + Q2
    ORDER = (0, NX - 1, 1, 2)

    me = lax.axis_index("ep")
    ty = lax.axis_index("tp")
    cx = me // 2
    cc = me % 2
    mate = cx * 2 + (1 - cc)
    rx = (cx + 1) % NX
    lx = (cx + NX - 1) % NX
    right = {"ep": rx * 2 + cc}
    left = {"ep": lx * 2 + cc}
    up = {"tp": (ty + 1) % TP}
    down = {"tp": (ty + TP - 1) % TP}
    partner = {"ep": mate}

    def remote(src, dst, ssem, rsem, dev):
        return pltpu.make_async_remote_copy(src_ref=src, dst_ref=dst, send_sem=ssem, recv_sem=rsem, device_id=dev, device_id_type=MESH)

    def wpair(slot, ra, rb, n):
        return (pltpu.make_async_copy(ra, ring.at[slot, pl.ds(0, n), pl.ds(0, BLK)], wsem.at[slot, 0]),
                pltpu.make_async_copy(rb, ring.at[slot, pl.ds(0, n), pl.ds(BLK, BLK)], wsem.at[slot, 1]))

    def cols(i, w=BLK):
        return pl.ds(pl.multiple_of(i * w, w), w)

    def chunk_w(q, slot):
        e, n = q // C1, q % C1
        return wpair(slot % NS, w1.at[e, :, cols(n)], w3.at[e, :, cols(n)], D)

    def chunk_e(q):
        return chunk_w(q, q)

    def chunk_a(i):
        return wpair((i + O_A) % NS, ws1.at[:, cols(i)], ws3.at[:, cols(i)], D)

    def chunk_b(i):
        return wpair((i + O_B) % NS, ws2.at[:, cols(2 * i)], ws2.at[:, cols(2 * i + 1)], FS)

    def chunk_1(q):
        return chunk_w(q, q + O_1)

    def chunk_2(q):
        b, p = q // PAIRS, q % PAIRS
        return wpair((q + O_2) % NS, w2.at[2 * p, :, cols(b)], w2.at[2 * p + 1, :, cols(b)], FF)

    def start(pair):
        pair[0].start()
        pair[1].start()

    def wait(pair):
        pair[0].wait()
        pair[1].wait()

    def start_at(i):
        bounds = ((0, O_A, chunk_e), (O_A, O_B, chunk_a), (O_B, O_1, chunk_b), (O_1, O_2, chunk_1), (O_2, total, chunk_2))
        for lo, hi, fn in bounds:
            if isinstance(i, int):
                if lo <= i < hi:
                    start(fn(i - lo))
            else:
                @pl.when((i >= lo) & (i < hi))
                def _(fn=fn, lo=lo):
                    start(fn(i - lo))

    own = pltpu.make_async_copy(tok, xg.at[me], own_sem)
    own.start()
    for i in range(NS - 1):
        start_at(i)

    barrier = pltpu.get_barrier_semaphore()
    for d in range(1, EP):
        pl.semaphore_signal(barrier, inc=1, device_id={"ep": (me + d) % EP}, device_id_type=MESH)
    for dev in (up, down):
        pl.semaphore_signal(barrier, inc=1, device_id=dev, device_id_type=MESH)
    own.wait()
    pl.semaphore_wait(barrier, EP + 1)

    lo_h, hi_h, all_h = pl.ds(0, H), pl.ds(H, H), pl.ds(0, NT)

    def xpart(dx, part):
        return xg.at[((cx + dx + NX) % NX) * 2 + cc, part, :]

    def xsend(k, dx, part, dev):
        ref = xpart(dx, part)
        return remote(ref, ref, xs.at[k], xr.at[k], dev)

    x_r0 = xsend(0, 0, lo_h, right)
    x_r1 = xsend(1, 0, hi_h, right)
    x_l1 = xsend(2, 0, hi_h, left)
    x_l0 = xsend(3, 0, lo_h, left)
    x_fr = xsend(4, -1, lo_h, right)
    x_fl = xsend(5, 1, hi_h, left)

    def psend(k, dx, part):
        ref = xpart(dx, part)
        return remote(ref, ref, ps.at[k], pr.at[k], partner)

    p_own = psend(0, 0, all_h)
    p_l = psend(1, -1, all_h)
    p_r = psend(2, 1, all_h)
    p_f0 = psend(3, 2, lo_h)
    p_f1 = psend(4, 2, hi_h)

    def ypart(j, part_start, n):
        return yg.at[pl.ds(j * NT + part_start, n), :]

    y_r0 = remote(xg.at[me, lo_h, :], ypart(0, 0, H), ys.at[0], yr.at[0], up)
    y_r1 = remote(xg.at[me, hi_h, :], ypart(0, H, H), ys.at[1], yr.at[1], up)
    y_l1 = remote(xg.at[me, hi_h, :], ypart(1, H, H), ys.at[2], yr.at[2], down)
    y_l0 = remote(xg.at[me, lo_h, :], ypart(1, 0, H), ys.at[3], yr.at[3], down)
    y_fr = remote(ypart(0, 0, H), ypart(2, 0, H), ys.at[4], yr.at[4], up)
    y_fl = remote(ypart(1, H, H), ypart(2, H, H), ys.at[5], yr.at[5], down)

    metas = [remote(mg.at[me], mg.at[me], ms.at[d - 1], mr.at[d - 1], {"ep": (me + d) % EP}) for d in range(1, EP)]

    d_mate = (me + EP - mate) % EP
    mate_meta = remote(mg.at[mate], mg.at[mate], ms.at[d_mate - 1], mr.at[d_mate - 1], partner)

    for c in (x_r0, x_l1, y_r0, y_l1, p_own, x_r1, x_l0, y_r1, y_l0):
        c.start()
    mg[me] = jnp.zeros((META, NT), F32)

    id_t = ids[...].astype(F32)
    slot_t = slots[...].astype(F32)
    limit = jnp.zeros_like(id_t)
    for e in range(NL * EP):
        limit = jnp.where(id_t == float(e), counts[0, e].astype(F32), limit)
    kept = (slot_t >= 0.0) & (slot_t < limit)
    mg[me, 0:TOPK, :] = jnp.where(kept, id_t * float(CAP) + slot_t, float(NL * EP * CAP))
    mg[me, 8:8 + TOPK, :] = jnp.where(kept, gates[...], 0.0)
    for c in metas:
        c.start()

    row_id = lax.broadcasted_iota(jnp.int32, (LROWS, NT), 0).astype(F32) + (me * LROWS).astype(F32)

    def gather(j, _):
        dx = (3 * j + 3 * (j // 2) - 2 * (j // 3)) % NX
        x0 = ((cx + dx) % NX) * 2
        for c in range(2):
            m = mg[x0 + c]
            pick = jnp.zeros((LROWS, NT), F32)
            wgt = jnp.zeros((LROWS, NT), F32)
            for t in range(TOPK):
                hit = m[t:t + 1, :] == row_id
                pick = jnp.where(hit, 1.0, pick)
                wgt = wgt + jnp.where(hit, m[8 + t:9 + t, :], 0.0)
            pick = pick.astype(BF)
            wt = jnp.transpose(wgt)
            hi = wt.astype(BF)
            rest = wt - hi.astype(F32)
            mid = rest.astype(BF)
            low = (rest - mid.astype(F32)).astype(BF)
            gm[x0 + c, :, 0:LROWS] = hi
            gm[x0 + c, :, LROWS:2 * LROWS] = mid
            gm[x0 + c, :, 2 * LROWS:3 * LROWS] = low
            if GK > 3 * LROWS:
                gm[x0 + c, :, 3 * LROWS:GK] = jnp.zeros((NT, GK - 3 * LROWS), BF)
            place = pl.ds(pl.multiple_of(j * PR + c * CAP, 16), CAP)
            for n in range(D // 512):
                part = slice(n * 512, (n + 1) * 512)
                got = dot(pick, xg[x0 + c, :, part]).astype(BF)
                for e in range(NL):
                    hr[e + 1, place, part] = got[e * CAP:(e + 1) * CAP, :]
        return 0

    def early(e, _):
        @pl.when(e == NE // 2)
        def _():
            relay()

        @pl.when(e == NE - 1)
        def _():
            x_r1.wait_recv()
            p_l.start()
            x_l0.wait_recv()
            p_r.start()

        for n in range(C1):
            q = e * C1 + n
            wait(chunk_e(q))
            start_at(q - 1 + NS)
            r = dot(hr[e + 1, 0:PR, :], ring[q % NS])
            hr[e, 0:PR, n * BLK:(n + 1) * BLK] = silu_mul(r[:, :BLK], r[:, BLK:])
        return 0

    def relay():
        x_r0.wait_recv()
        x_fr.start()
        x_l1.wait_recv()
        x_fl.start()
        y_r0.wait_recv()
        y_fr.start()
        y_l1.wait_recv()
        y_fl.start()

    def shared():
        def stretch(lo, hi, free):
            for i in range(lo, hi):
                wait(chunk_a(i - O_A) if i < O_B else chunk_b(i - O_B))
            for i in range(free, lo):
                start_at(i + NS)
            for i in range(lo, hi):
                if i < O_B:
                    here = slice((i - O_A) * BLK, (i - O_A + 1) * BLK)
                    r = dot(yg[...], ring[i % NS])
                    sh[NT:, here] = silu_mul(r[:, :BLK], r[:, BLK:])
                    r = dot(xg[me], ring[i % NS])
                    sh[0:NT, here] = silu_mul(r[:, :BLK], r[:, BLK:])
                else:
                    b = i - O_B
                    r = dot(sh[...], ring[i % NS, 0:FS, :])
                    here = slice(2 * b * BLK, (2 * b + 2) * BLK)
                    acc[:, here] = xg[me, :, here].astype(F32) + r[0:NT]
                    for j in range(3):
                        for m in range(2):
                            pb[2 * b + m, j] = r[(j + 1) * NT:(j + 2) * NT, m * BLK:(m + 1) * BLK]

        stretch(O_A, O_B, O_A - 1)
        stretch(O_B, O_B + 3, O_A)
        stretch(O_B + 3, O_1, O_B)

    def head():
        mate_meta.wait_recv()
        p_own.wait_recv()
        lax.fori_loop(0, 1, gather, 0)
        lax.fori_loop(0, NE, early, 0)
        for d in range(1, EP):
            @pl.when(d != d_mate)
            def _(d=d):
                metas[d - 1].wait_recv()

        y_r1.wait_recv()
        y_l0.wait_recv()
        p_l.wait_recv()
        p_r.wait_recv()
        lax.fori_loop(1, NX - 1, gather, 0)
        x_fr.wait_recv()
        p_f0.start()
        x_fl.wait_recv()
        p_f1.start()
        y_fr.wait_recv()
        y_fl.wait_recv()
        shared()
        for c in y_halves:
            c.start()
        p_f0.wait_recv()
        p_f1.wait_recv()
        lax.fori_loop(NX - 1, NX, gather, 0)

    def y_half(k, dev):
        return remote(pb.at[:, 2, pl.ds(k * H, H), :], yfar.at[k], ysend.at[k], yrecv.at[k], dev)

    def y_full(k, j, dev):
        return remote(pb.at[:, j], fin.at[k], ysend.at[2 + k], yrecv.at[2 + k], dev)

    y_halves = (y_half(0, up), y_half(1, down))
    y_fulls = (y_full(0, 1, up), y_full(1, 0, down))
    def y_step2():
        for c in y_halves:
            c.wait()

        def add(i, _):
            pb[i, 1, 0:H, :] += yfar[0, i]
            pb[i, 0, H:NT, :] += yfar[1, i]
            return 0

        lax.fori_loop(0, NB, add, 0)
        for c in y_fulls:
            c.start()

    def y_step3():
        for c in y_fulls:
            c.wait()

        def add(i, _):
            acc[:, cols(i)] += fin[0, i] + fin[1, i]
            return 0

        lax.fori_loop(0, NB, add, 0)

    def finish(r, r0, e, n):
        hr[e, r0:ROWS, n * BLK:(n + 1) * BLK] = silu_mul(r[:, :BLK], r[:, BLK:])

    def first(r0, e0, e, _):
        if e0 == 0:
            @pl.when(e == NE - 1)
            def _():
                y_step2()

        for h in range(C1 // G1):
            q = e * C1 + h * G1
            for i in range(G1):
                wait(chunk_1(q + i))
            for i in range(G1):
                ahead = q + NS - G1 + i
                past = (h - 1) * G1 + NS + i - C1
                if e0 == 0 or past < 0:
                    start(chunk_1(ahead))
                else:
                    @pl.when(ahead < Q1)
                    def _(ahead=ahead):
                        start(chunk_1(ahead))

                    @pl.when(ahead >= Q1)
                    def _(past=past):
                        start(chunk_2(past))
            rows = hr[e + 1, r0:ROWS, :]
            for i in range(G1):
                n = h * G1 + i
                r = dot(rows, ring[(O_1 + n) % NS])
                if i == 0:
                    if h:
                        finish(gu[r0:ROWS], r0, e, n - 1)
                    else:
                        finish(gu[r0:ROWS], r0, jnp.maximum(e - 1, e0), C1 - 1)
                if i + 1 < G1:
                    finish(r, r0, e, n)
                else:
                    gu[r0:ROWS] = r
        return 0

    def middle():
        lax.fori_loop(0, NE, functools.partial(first, PR, 0), 0)
        finish(gu[PR:ROWS], PR, NE - 1, C1 - 1)
        lax.fori_loop(NE, NL, functools.partial(first, 0, NE), 0)
        finish(gu[...], 0, NL - 1, C1 - 1)
        y_step3()

    def to_mate(b):
        return remote(sb.at[b % 2], d2d.at[b % 2], dsend.at[b], drecv.at[b], partner)

    def half(b, k, dev):
        return remote(pb.at[b, 3, pl.ds(k * H, H), :], far.at[k, b], fsend.at[k, b], frecv.at[k, b], dev)

    def full(b, k, dev):
        return remote(pb.at[b, 2 - k], fin.at[k, b], nsend.at[k, b], nrecv.at[k, b], dev)

    def step_b(b):
        to_mate(b).wait_recv()
        pb[b] += d2d[b % 2]
        half(b, 0, right).start()
        half(b, 1, left).start()

    def step_c(b):
        half(b, 0, right).wait_recv()
        half(b, 1, left).wait_recv()
        pb[b, 2, 0:H, :] += far[0, b]
        pb[b, 1, H:NT, :] += far[1, b]
        full(b, 0, right).start()
        full(b, 1, left).start()

    def step_d(b, _):
        full(b, 0, right).wait_recv()
        full(b, 1, left).wait_recv()
        out[:, cols(b)] = (acc[:, cols(b)] + pb[b, 0] + fin[0, b] + fin[1, b]).astype(BF)
        return 0

    side = slice(FF, FF + BLK)

    def combine(b):
        half_x = NX // 2
        for i in range(2):
            par = (1 - cc, cc)[i]
            for j in range(NX):
                src = ((cx + ORDER[j]) % NX) * 2 + par
                place = pl.ds(pl.multiple_of((2 * j + par) * CAP, 16), CAP)
                r = [hr[e, place, side] for e in range(NL)] * 3
                if GK > 3 * LROWS:
                    r.append(jnp.zeros((GK - 3 * LROWS, BLK), BF))
                v = dot(gm[src], jnp.concatenate(r, axis=0))
                if i == 0:
                    sb[b % 2, j] = v
                else:
                    pb[b, j] = v

    def pairs(b, h):
        q = b * PAIRS + h * G2
        for i in range(G2):
            wait(chunk_2(q + i))
        for i in range(G2):
            @pl.when(q + NS - G2 + i < Q2)
            def _(i=i):
                start(chunk_2(q + NS - G2 + i))

    def rows_out(b, h):
        q = b * PAIRS + h * G2
        for i in range(G2):
            slot = (q + O_2 + i) % NS
            for m in range(2):
                e = 2 * (h * G2 + i) + m
                hr[e, :, side] = dot(hr[e, :, 0:FF], ring[slot, 0:FF, m * BLK:(m + 1) * BLK]).astype(BF)

    def second(b, _):
        pairs(b, 0)
        rows_out(b, 0)

        @pl.when(b >= 1)
        def _():
            step_b(b - 1)

        @pl.when(b >= 2)
        def _():
            step_c(b - 2)
            to_mate(b - 2).wait_send()

        @pl.when(b >= 5)
        def _():
            step_d(b - 5, 0)

        pairs(b, 1)
        rows_out(b, 1)
        combine(b)
        to_mate(b).start()
        return 0

    head()
    middle()
    lax.fori_loop(0, NB, second, 0)
    step_b(NB - 1)
    step_c(NB - 2)
    step_c(NB - 1)
    lax.fori_loop(NB - 5, NB, step_d, 0)

    for c in metas:
        c.wait_send()
    for c in (x_r0, x_r1, x_l1, x_l0, x_fr, x_fl, p_own, p_l, p_r, p_f0, p_f1, y_r0, y_r1, y_l1, y_l0, y_fr, y_fl):
        c.wait_send()
    to_mate(NB - 2).wait_send()
    to_mate(NB - 1).wait_send()

    def drain(b, _):
        half(b, 0, right).wait_send()
        half(b, 1, left).wait_send()
        full(b, 0, right).wait_send()
        full(b, 1, left).wait_send()
        return 0

    lax.fori_loop(0, NB, drain, 0)


def solution(mesh):
    ep_size = mesh.shape["ep"]
    tp_size = mesh.shape["tp"]
    row_spec = P(("data", "ep", "tp"), None)
    expert_spec = P("ep", None, None)

    def layer_body(tokens, expert_ids, gate_vals, slot_ids, send_counts, shared_w1, shared_w3, shared_w2, expert_w1, expert_w3, expert_w2):
        n_tok, d_model = tokens.shape
        top_k = expert_ids.shape[1]
        n_local, _, width = expert_w1.shape
        shared_width = shared_w1.shape[1]
        n_exp = n_local * ep_size
        capacity = capacity_rows(n_tok, top_k, n_exp)
        ns = 6
        nb = d_model // BLK
        local_rows = n_local * capacity
        cfg = (ep_size, tp_size, n_tok, d_model, width, shared_width, n_local, capacity, top_k, ns)
        half = n_tok // 2
        nx = ep_size // 2
        hbm = pl.BlockSpec(memory_space=pl.ANY)
        vmem = pl.BlockSpec(memory_space=pltpu.VMEM)
        dma = pltpu.SemaphoreType.DMA
        return pl.pallas_call(
            functools.partial(layer_kernel, cfg),
            out_shape=jax.ShapeDtypeStruct((n_tok, d_model), BF),
            in_specs=[hbm, vmem, vmem, vmem, pl.BlockSpec(memory_space=pltpu.SMEM)] + [hbm] * 6,
            out_specs=vmem,
            scratch_shapes=[
                pltpu.VMEM((n_local + 1, ep_size * capacity, d_model), BF),
                pltpu.VMEM((ep_size, n_tok, d_model), BF),
                pltpu.VMEM(((tp_size - 1) * n_tok, d_model), BF),
                pltpu.VMEM((ep_size, META, n_tok), F32),
                pltpu.VMEM((nb, nx, n_tok, BLK), F32),
                pltpu.VMEM((2, nx, n_tok, BLK), F32),
                pltpu.VMEM((2, nx, n_tok, BLK), F32),
                pltpu.VMEM((2, nb, half, BLK), F32),
                pltpu.VMEM((2, nb, n_tok, BLK), F32),
                pltpu.VMEM((2, nb, half, BLK), F32),
                pltpu.VMEM((n_tok, d_model), F32),
                pltpu.VMEM((tp_size * n_tok, shared_width), BF),
                pltpu.VMEM((ep_size * capacity, 2 * BLK), F32),
                                pltpu.VMEM((ep_size, n_tok, -(-3 * local_rows // BLK) * BLK), BF),
                pltpu.VMEM((ns, d_model, 2 * BLK), BF),
                dma, dma((6,)), dma((6,)), dma((5,)), dma((5,)), dma((ep_size - 1,)), dma((ep_size - 1,)),
                dma((6,)), dma((6,)), dma((ns, 2)),
                dma((4,)), dma((4,)), dma((nb,)), dma((nb,)), dma((2, nb)), dma((2, nb)), dma((2, nb)), dma((2, nb)),
            ],
            compiler_params=pltpu.CompilerParams(collective_id=0, has_side_effects=True, vmem_limit_bytes=67043328),
            cost_estimate=pl.CostEstimate(flops=80_000_000_000, bytes_accessed=200_000_000, transcendentals=0),
            name="moe_layer",
        )(tokens, expert_ids.T, slot_ids.T, gate_vals.T, send_counts, shared_w1, shared_w3, shared_w2, expert_w1, expert_w3, expert_w2)

    return jax.shard_map(
        layer_body,
        mesh=mesh,
        in_specs=(row_spec, row_spec, row_spec, row_spec, row_spec, P(None, "tp"), P(None, "tp"), P("tp", None), expert_spec, expert_spec, expert_spec),
        out_specs=row_spec,
        check_vma=False,
    )
```

```python
import functools

import jax
import jax.numpy as jnp
from jax import lax
from jax.experimental import pallas as pl
from jax.experimental.pallas import tpu as pltpu
from jax.sharding import PartitionSpec as P

CAP_FACTOR = 4
BF = jnp.bfloat16
F32 = jnp.float32
MESH = pl.DeviceIdType.MESH
BLK = 256
META = 16


def capacity_rows(n_tok, top_k, n_exp):
    return min(n_tok, ((CAP_FACTOR * n_tok * top_k // n_exp + 7) // 8) * 8)


def silu_mul(g, u):
    return (g * (1.0 / (1.0 + jnp.exp(-g))) * u).astype(BF)


def dot(a, b):
    return jnp.dot(a, b, preferred_element_type=F32)


def layer_kernel(cfg, tok, ids, slots, gates, counts, ws1, ws3, ws2, w1, w3, w2, out,
                 hr, xg, yg, mg, pb, sb, d2d, far, fin, yfar, yfin, acc, sh, gu, gm, ring,
                 own_sem, xs, xr, ps, pr, ms, mr, ys, yr, wsem,
                 ysend, yrecv, dsend, drecv, fsend, frecv, nsend, nrecv):
    EP, TP, NT, D, FF, FS, NL, CAP, TOPK, NS = cfg
    ROWS = EP * CAP
    LROWS = NL * CAP
    H = NT // 2
    NX = EP // 2
    NB = D // BLK
    C1 = FF // BLK
    Q1 = NL * C1
    PAIRS = NL // 2
    Q2 = NB * PAIRS
    SA = FS // BLK
    SB = D // (2 * BLK)
    K1 = D // BLK
    K2 = FF // BLK
    KG = -(-3 * LROWS // BLK)
    GK = KG * BLK
    KS = FS // BLK
    NE = NL // 2
    G1 = C1 // 3
    G2 = PAIRS // 2
    QE = NE * C1
    PR = 2 * CAP
    O_A = QE
    O_B = O_A + SA
    O_1 = O_B + SB
    O_2 = O_1 + Q1
    total = O_2 + Q2
    ORDER = (0, NX - 1, 1, 2)

    me = lax.axis_index("ep")
    ty = lax.axis_index("tp")
    cx = me // 2
    cc = me % 2
    mate = cx * 2 + (1 - cc)
    rx = (cx + 1) % NX
    lx = (cx + NX - 1) % NX
    right = {"ep": rx * 2 + cc}
    left = {"ep": lx * 2 + cc}
    up = {"tp": (ty + 1) % TP}
    down = {"tp": (ty + TP - 1) % TP}
    partner = {"ep": mate}

    def remote(src, dst, ssem, rsem, dev):
        return pltpu.make_async_remote_copy(src_ref=src, dst_ref=dst, send_sem=ssem, recv_sem=rsem, device_id=dev, device_id_type=MESH)

    def wpair(slot, ra, rb, n):
        return (pltpu.make_async_copy(ra, ring.at[slot, pl.ds(0, n), pl.ds(0, BLK)], wsem.at[slot, 0]),
                pltpu.make_async_copy(rb, ring.at[slot, pl.ds(0, n), pl.ds(BLK, BLK)], wsem.at[slot, 1]))

    def cols(i, w=BLK):
        return pl.ds(pl.multiple_of(i * w, w), w)

    def chunk_w(q, slot):
        e, n = q // C1, q % C1
        return wpair(slot % NS, w1.at[e, :, cols(n)], w3.at[e, :, cols(n)], D)

    def chunk_e(q):
        return chunk_w(q, q)

    def chunk_a(i):
        return wpair((i + O_A) % NS, ws1.at[:, cols(i)], ws3.at[:, cols(i)], D)

    def chunk_b(i):
        return wpair((i + O_B) % NS, ws2.at[:, cols(2 * i)], ws2.at[:, cols(2 * i + 1)], FS)

    def chunk_1(q):
        return chunk_w(q, q + O_1)

    def chunk_2(q):
        b, p = q // PAIRS, q % PAIRS
        return wpair((q + O_2) % NS, w2.at[2 * p, :, cols(b)], w2.at[2 * p + 1, :, cols(b)], FF)

    def start(pair):
        pair[0].start()
        pair[1].start()

    def wait(pair):
        pair[0].wait()
        pair[1].wait()

    def start_at(i):
        bounds = ((0, O_A, chunk_e), (O_A, O_B, chunk_a), (O_B, O_1, chunk_b), (O_1, O_2, chunk_1), (O_2, total, chunk_2))
        for lo, hi, fn in bounds:
            if isinstance(i, int):
                if lo <= i < hi:
                    start(fn(i - lo))
            else:
                @pl.when((i >= lo) & (i < hi))
                def _(fn=fn, lo=lo):
                    start(fn(i - lo))

    own = pltpu.make_async_copy(tok, xg.at[me], own_sem)
    own.start()

    barrier = pltpu.get_barrier_semaphore()
    for d in range(1, EP):
        pl.semaphore_signal(barrier, inc=1, device_id={"ep": (me + d) % EP}, device_id_type=MESH)
    for dev in (up, down):
        pl.semaphore_signal(barrier, inc=1, device_id=dev, device_id_type=MESH)
    own.wait()
    for i in range(NS - 1):
        start_at(i)
    pl.semaphore_wait(barrier, EP + 1)

    lo_h, hi_h, all_h = pl.ds(0, H), pl.ds(H, H), pl.ds(0, NT)

    def xpart(dx, part):
        return xg.at[((cx + dx + NX) % NX) * 2 + cc, part, :]

    def xsend(k, dx, part, dev):
        ref = xpart(dx, part)
        return remote(ref, ref, xs.at[k], xr.at[k], dev)

    x_r0 = xsend(0, 0, lo_h, right)
    x_r1 = xsend(1, 0, hi_h, right)
    x_l1 = xsend(2, 0, hi_h, left)
    x_l0 = xsend(3, 0, lo_h, left)
    x_fr = xsend(4, -1, lo_h, right)
    x_fl = xsend(5, 1, hi_h, left)

    def psend(k, dx, part):
        ref = xpart(dx, part)
        return remote(ref, ref, ps.at[k], pr.at[k], partner)

    p_own = psend(0, 0, all_h)
    p_l = psend(1, -1, all_h)
    p_r = psend(2, 1, all_h)
    p_f0 = psend(3, 2, lo_h)
    p_f1 = psend(4, 2, hi_h)

    def ypart(j, part_start, n):
        return yg.at[pl.ds(j * NT + part_start, n), :]

    y_r0 = remote(xg.at[me, lo_h, :], ypart(0, 0, H), ys.at[0], yr.at[0], up)
    y_r1 = remote(xg.at[me, hi_h, :], ypart(0, H, H), ys.at[1], yr.at[1], up)
    y_l1 = remote(xg.at[me, hi_h, :], ypart(1, H, H), ys.at[2], yr.at[2], down)
    y_l0 = remote(xg.at[me, lo_h, :], ypart(1, 0, H), ys.at[3], yr.at[3], down)
    y_fr = remote(ypart(0, 0, H), ypart(2, 0, H), ys.at[4], yr.at[4], up)
    y_fl = remote(ypart(1, H, H), ypart(2, H, H), ys.at[5], yr.at[5], down)

    metas = [remote(mg.at[me], mg.at[me], ms.at[d - 1], mr.at[d - 1], {"ep": (me + d) % EP}) for d in range(1, EP)]

    d_mate = (me + EP - mate) % EP
    mate_meta = remote(mg.at[mate], mg.at[mate], ms.at[d_mate - 1], mr.at[d_mate - 1], partner)

    for c in (x_r0, x_l1, y_r0, y_l1, p_own, x_r1, x_l0, y_r1, y_l0):
        c.start()
    mg[me] = jnp.zeros((META, NT), F32)

    id_t = ids[...].astype(F32)
    slot_t = slots[...].astype(F32)
    limit = jnp.zeros_like(id_t)
    for e in range(NL * EP):
        limit = jnp.where(id_t == float(e), counts[0, e].astype(F32), limit)
    kept = (slot_t >= 0.0) & (slot_t < limit)
    mg[me, 0:TOPK, :] = jnp.where(kept, id_t * float(CAP) + slot_t, float(NL * EP * CAP))
    mg[me, 8:8 + TOPK, :] = jnp.where(kept, gates[...], 0.0)
    for c in metas:
        c.start()

    row_id = lax.broadcasted_iota(jnp.int32, (LROWS, NT), 0).astype(F32) + (me * LROWS).astype(F32)

    def gather(j, _):
        dx = (3 * j + 3 * (j // 2) - 2 * (j // 3)) % NX
        x0 = ((cx + dx) % NX) * 2
        for c in range(2):
            m = mg[x0 + c]
            pick = jnp.zeros((LROWS, NT), F32)
            wgt = jnp.zeros((LROWS, NT), F32)
            for t in range(TOPK):
                hit = m[t:t + 1, :] == row_id
                pick = jnp.where(hit, 1.0, pick)
                wgt = wgt + jnp.where(hit, m[8 + t:9 + t, :], 0.0)
            pick = pick.astype(BF)
            wt = jnp.transpose(wgt)
            hi = wt.astype(BF)
            rest = wt - hi.astype(F32)
            mid = rest.astype(BF)
            low = (rest - mid.astype(F32)).astype(BF)
            gm[x0 + c, :, 0:LROWS] = hi
            gm[x0 + c, :, LROWS:2 * LROWS] = mid
            gm[x0 + c, :, 2 * LROWS:3 * LROWS] = low
            if GK > 3 * LROWS:
                gm[x0 + c, :, 3 * LROWS:GK] = jnp.zeros((NT, GK - 3 * LROWS), BF)
            place = pl.ds(pl.multiple_of(j * PR + c * CAP, 16), CAP)
            for n in range(D // 512):
                part = slice(n * 512, (n + 1) * 512)
                got = dot(pick, xg[x0 + c, :, part]).astype(BF)
                for e in range(NL):
                    hr[e + 1, place, part] = got[e * CAP:(e + 1) * CAP, :]
        return 0

    def early(e, _):
        @pl.when(e == NE // 2)
        def _():
            relay()

        @pl.when(e == NE - 1)
        def _():
            x_r1.wait_recv()
            p_l.start()
            x_l0.wait_recv()
            p_r.start()

        for n in range(C1):
            q = e * C1 + n
            wait(chunk_e(q))
            start_at(q - 1 + NS)
            r = dot(hr[e + 1, 0:PR, :], ring[q % NS])
            hr[e, 0:PR, n * BLK:(n + 1) * BLK] = silu_mul(r[:, :BLK], r[:, BLK:])
        return 0

    def relay():
        x_r0.wait_recv()
        x_fr.start()
        x_l1.wait_recv()
        x_fl.start()
        y_r0.wait_recv()
        y_fr.start()
        y_l1.wait_recv()
        y_fl.start()

    def shared():
        def stretch(lo, hi, free):
            for i in range(lo, hi):
                wait(chunk_a(i - O_A) if i < O_B else chunk_b(i - O_B))
            for i in range(free, lo):
                start_at(i + NS)
            for i in range(lo, hi):
                if i < O_B:
                    here = slice((i - O_A) * BLK, (i - O_A + 1) * BLK)
                    r = dot(yg[...], ring[i % NS])
                    sh[NT:, here] = silu_mul(r[:, :BLK], r[:, BLK:])
                    r = dot(xg[me], ring[i % NS])
                    sh[0:NT, here] = silu_mul(r[:, :BLK], r[:, BLK:])
                else:
                    b = i - O_B
                    r = dot(sh[...], ring[i % NS, 0:FS, :])
                    here = slice(2 * b * BLK, (2 * b + 2) * BLK)
                    acc[:, here] = xg[me, :, here].astype(F32) + r[0:NT]
                    for j in range(3):
                        for m in range(2):
                            pb[2 * b + m, j] = r[(j + 1) * NT:(j + 2) * NT, m * BLK:(m + 1) * BLK]

        stretch(O_A, O_B, O_A - 1)
        stretch(O_B, O_B + 3, O_A)
        stretch(O_B + 3, O_1, O_B)

    def head():
        mate_meta.wait_recv()
        p_own.wait_recv()
        lax.fori_loop(0, 1, gather, 0)
        lax.fori_loop(0, NE, early, 0)
        for d in range(1, EP):
            @pl.when(d != d_mate)
            def _(d=d):
                metas[d - 1].wait_recv()

        y_r1.wait_recv()
        y_l0.wait_recv()
        p_l.wait_recv()
        p_r.wait_recv()
        lax.fori_loop(1, NX - 1, gather, 0)
        x_fr.wait_recv()
        p_f0.start()
        x_fl.wait_recv()
        p_f1.start()
        y_fr.wait_recv()
        y_fl.wait_recv()
        shared()
        for c in y_halves + y_plain:
            c.start()
        p_f0.wait_recv()
        p_f1.wait_recv()
        lax.fori_loop(NX - 1, NX, gather, 0)

    def y_half(k, dev):
        return remote(pb.at[:, 2, pl.ds(k * H, H), :], yfar.at[k], ysend.at[k], yrecv.at[k], dev)

    def y_part(i, j, part, dev):
        return remote(pb.at[:, j, part, :], yfin.at[1 - j, :, part, :], ysend.at[2 + i], yrecv.at[2 + i], dev)

    y_halves = (y_half(0, up), y_half(1, down))
    y_plain = (y_part(0, 1, hi_h, up), y_part(1, 0, lo_h, down))
    y_added = (y_part(2, 1, lo_h, up), y_part(3, 0, hi_h, down))

    def y_step2():
        for c in y_halves:
            c.wait()

        def add(i, _):
            pb[i, 1, 0:H, :] += yfar[0, i]
            pb[i, 0, H:NT, :] += yfar[1, i]
            return 0

        lax.fori_loop(0, NB, add, 0)
        for c in y_added:
            c.start()

    def y_step3():
        for c in y_plain + y_added:
            c.wait()

        def add(i, _):
            acc[:, cols(i)] += yfin[0, i] + yfin[1, i]
            return 0

        lax.fori_loop(0, NB, add, 0)

    def finish(r, r0, e, n):
        hr[e, r0:ROWS, n * BLK:(n + 1) * BLK] = silu_mul(r[:, :BLK], r[:, BLK:])

    def first(r0, e0, e, _):
        if e0:
            @pl.when(e == e0)
            def _():
                y_step2()

        for h in range(C1 // G1):
            q = e * C1 + h * G1
            for i in range(G1):
                wait(chunk_1(q + i))
            for i in range(G1):
                ahead = q + NS - G1 + i
                past = (h - 1) * G1 + NS + i - C1
                if e0 == 0 or past < 0:
                    start(chunk_1(ahead))
                else:
                    @pl.when(ahead < Q1)
                    def _(ahead=ahead):
                        start(chunk_1(ahead))

                    @pl.when(ahead >= Q1)
                    def _(past=past):
                        start(chunk_2(past))
            rows = hr[e + 1, r0:ROWS, :]
            for i in range(G1):
                n = h * G1 + i
                r = dot(rows, ring[(O_1 + n) % NS])
                if i == 0:
                    if h:
                        finish(gu[r0:ROWS], r0, e, n - 1)
                    else:
                        finish(gu[r0:ROWS], r0, jnp.maximum(e - 1, e0), C1 - 1)
                if i + 1 < G1:
                    finish(r, r0, e, n)
                else:
                    gu[r0:ROWS] = r
        return 0

    def middle():
        lax.fori_loop(0, NE, functools.partial(first, PR, 0), 0)
        finish(gu[PR:ROWS], PR, NE - 1, C1 - 1)
        lax.fori_loop(NE, NL, functools.partial(first, 0, NE), 0)
        finish(gu[...], 0, NL - 1, C1 - 1)
        y_step3()

    def to_mate(b):
        return remote(sb.at[b % 2], d2d.at[b % 2], dsend.at[b % 2], drecv.at[b], partner)

    def half(b, k, dev):
        return remote(pb.at[b, 3, pl.ds(k * H, H), :], far.at[k, b], fsend.at[k, b % 2], frecv.at[k, b], dev)

    def part(b, i, dev):
        k = i % 2
        rows = (hi_h, lo_h, lo_h, hi_h)[i]
        return remote(pb.at[b, 2 - k, rows, :], fin.at[k, b, rows, :], nsend.at[i, b % 2], nrecv.at[i, b], dev)

    sides = (right, left, right, left)

    def sent_b(b):
        half(b, 0, right).wait_send()
        half(b, 1, left).wait_send()
        for i in (0, 1):
            part(b, i, sides[i]).wait_send()

    def sent_c(b):
        for i in (2, 3):
            part(b, i, sides[i]).wait_send()

    def step_b(b):
        to_mate(b).wait_recv()
        pb[b] += d2d[b % 2]
        if isinstance(b, int):
            sent_b(b - 2)
        else:
            @pl.when(b >= 2)
            def _():
                sent_b(b - 2)
        half(b, 0, right).start()
        half(b, 1, left).start()
        for i in (0, 1):
            part(b, i, sides[i]).start()

    def step_c(b):
        half(b, 0, right).wait_recv()
        half(b, 1, left).wait_recv()
        pb[b, 2, 0:H, :] += far[0, b]
        pb[b, 1, H:NT, :] += far[1, b]
        if isinstance(b, int):
            sent_c(b - 2)
        else:
            @pl.when(b >= 2)
            def _():
                sent_c(b - 2)
        for i in (2, 3):
            part(b, i, sides[i]).start()

    def step_d(b, _):
        for i in range(4):
            part(b, i, sides[i]).wait_recv()
        out[:, cols(b)] = (acc[:, cols(b)] + pb[b, 0] + fin[0, b] + fin[1, b]).astype(BF)
        return 0

    side = slice(FF, FF + BLK)

    def combine(b):
        half_x = NX // 2
        for i in range(2):
            par = (1 - cc, cc)[i]
            for j in range(NX):
                src = ((cx + ORDER[j]) % NX) * 2 + par
                place = pl.ds(pl.multiple_of((2 * j + par) * CAP, 16), CAP)
                r = [hr[e, place, side] for e in range(NL)] * 3
                if GK > 3 * LROWS:
                    r.append(jnp.zeros((GK - 3 * LROWS, BLK), BF))
                v = dot(gm[src], jnp.concatenate(r, axis=0))
                if i == 0:
                    sb[b % 2, j] = v
                else:
                    pb[b, j] = v
            if i == 0:
                to_mate(b).start()

    def pairs(b, h):
        q = b * PAIRS + h * G2
        for i in range(G2):
            wait(chunk_2(q + i))
        for i in range(G2):
            @pl.when(q + NS - G2 + i < Q2)
            def _(i=i):
                start(chunk_2(q + NS - G2 + i))

    def rows_out(b, h):
        q = b * PAIRS + h * G2
        for i in range(G2):
            slot = (q + O_2 + i) % NS
            for m in range(2):
                e = 2 * (h * G2 + i) + m
                hr[e, :, side] = dot(hr[e, :, 0:FF], ring[slot, 0:FF, m * BLK:(m + 1) * BLK]).astype(BF)

    def second(b, _):
        pairs(b, 0)
        rows_out(b, 0)

        @pl.when(b >= 1)
        def _():
            step_b(b - 1)

        @pl.when(b >= 2)
        def _():
            step_c(b - 2)
            to_mate(b - 2).wait_send()

        @pl.when(b >= 5)
        def _():
            step_d(b - 5, 0)

        pairs(b, 1)
        rows_out(b, 1)
        combine(b)
        return 0

    head()
    middle()
    lax.fori_loop(0, NB, second, 0)
    step_b(NB - 1)
    step_c(NB - 2)
    step_c(NB - 1)
    lax.fori_loop(NB - 5, NB, step_d, 0)

    for c in metas:
        c.wait_send()
    for c in (x_r0, x_r1, x_l1, x_l0, x_fr, x_fl, p_own, p_l, p_r, p_f0, p_f1, y_r0, y_r1, y_l1, y_l0, y_fr, y_fl):
        c.wait_send()
    to_mate(NB - 2).wait_send()
    to_mate(NB - 1).wait_send()

    for b in (NB - 2, NB - 1):
        sent_b(b)
        sent_c(b)


def solution(mesh):
    ep_size = mesh.shape["ep"]
    tp_size = mesh.shape["tp"]
    row_spec = P(("data", "ep", "tp"), None)
    expert_spec = P("ep", None, None)

    def layer_body(tokens, expert_ids, gate_vals, slot_ids, send_counts, shared_w1, shared_w3, shared_w2, expert_w1, expert_w3, expert_w2):
        n_tok, d_model = tokens.shape
        top_k = expert_ids.shape[1]
        n_local, _, width = expert_w1.shape
        shared_width = shared_w1.shape[1]
        n_exp = n_local * ep_size
        capacity = capacity_rows(n_tok, top_k, n_exp)
        ns = 6
        nb = d_model // BLK
        local_rows = n_local * capacity
        cfg = (ep_size, tp_size, n_tok, d_model, width, shared_width, n_local, capacity, top_k, ns)
        half = n_tok // 2
        nx = ep_size // 2
        hbm = pl.BlockSpec(memory_space=pl.ANY)
        vmem = pl.BlockSpec(memory_space=pltpu.VMEM)
        dma = pltpu.SemaphoreType.DMA
        return pl.pallas_call(
            functools.partial(layer_kernel, cfg),
            out_shape=jax.ShapeDtypeStruct((n_tok, d_model), BF),
            in_specs=[hbm, vmem, vmem, vmem, pl.BlockSpec(memory_space=pltpu.SMEM)] + [hbm] * 6,
            out_specs=vmem,
            scratch_shapes=[
                pltpu.VMEM((n_local + 1, ep_size * capacity, d_model), BF),
                pltpu.VMEM((ep_size, n_tok, d_model), BF),
                pltpu.VMEM(((tp_size - 1) * n_tok, d_model), BF),
                pltpu.VMEM((ep_size, META, n_tok), F32),
                pltpu.VMEM((nb, nx, n_tok, BLK), F32),
                pltpu.VMEM((2, nx, n_tok, BLK), F32),
                pltpu.VMEM((2, nx, n_tok, BLK), F32),
                pltpu.VMEM((2, nb, half, BLK), F32),
                pltpu.VMEM((2, nb, n_tok, BLK), F32),
                pltpu.VMEM((2, nb, half, BLK), F32),
                pltpu.VMEM((2, nb, n_tok, BLK), F32),
                pltpu.VMEM((n_tok, d_model), F32),
                pltpu.VMEM((tp_size * n_tok, shared_width), BF),
                pltpu.VMEM((ep_size * capacity, 2 * BLK), F32),
                                pltpu.VMEM((ep_size, n_tok, -(-3 * local_rows // BLK) * BLK), BF),
                pltpu.VMEM((ns, d_model, 2 * BLK), BF),
                dma, dma((6,)), dma((6,)), dma((5,)), dma((5,)), dma((ep_size - 1,)), dma((ep_size - 1,)),
                dma((6,)), dma((6,)), dma((ns, 2)),
                dma((6,)), dma((6,)), dma((2,)), dma((nb,)), dma((2, 2)), dma((2, nb)), dma((4, 2)), dma((4, nb)),
            ],
            compiler_params=pltpu.CompilerParams(collective_id=0, has_side_effects=True, vmem_limit_bytes=67043328),
            cost_estimate=pl.CostEstimate(flops=80_000_000_000, bytes_accessed=200_000_000, transcendentals=0),
            name="moe_layer",
        )(tokens, expert_ids.T, slot_ids.T, gate_vals.T, send_counts, shared_w1, shared_w3, shared_w2, expert_w1, expert_w3, expert_w2)

    return jax.shard_map(
        layer_body,
        mesh=mesh,
        in_specs=(row_spec, row_spec, row_spec, row_spec, row_spec, P(None, "tp"), P(None, "tp"), P("tp", None), expert_spec, expert_spec, expert_spec),
        out_specs=row_spec,
        check_vma=False,
    )
```
